128 devices in a mesh: rep: 2 (over core), dp: 64 (over x, y, z).
Axes of the slice: x: 4, y: 4, z: 4, core: 2. Of those that a mesh axis runs over, the one named last changes fastest.
Arguments:
- x: bfloat16 [128, 2048, 1024], P(('rep', 'dp')), parts along dimension 0
- dy: bfloat16 [128, 2048, 1024], P(('rep', 'dp')), parts along dimension 0
- w_gate: bfloat16 [2, 1024, 6144], P(None, 'dp')
- w_up: bfloat16 [2, 1024, 6144], P(None, 'dp')
- w_down: bfloat16 [2, 6144, 1024], P(None, 'dp')
Outputs:
- output 1: bfloat16 [128, 2048, 1024], P(('rep', 'dp')), parts along dimension 0
- output 2: bfloat16 [4, 1024, 6144], P('rep', 'dp'), parts along dimension 0
- output 3: bfloat16 [4, 1024, 6144], P('rep', 'dp'), parts along dimension 0
- output 4: bfloat16 [4, 6144, 1024], P('rep', 'dp'), parts along dimension 0
There are 2 independent parts. The reference program is written for one: setup_inputs(seed, part) draws one part's arguments, and reference() takes and returns one part's arrays. A program takes and returns all parts, laid end to end along the dimension named above; an argument that names none is the same for every part.
All inputs are finite; a program needn't handle non-finite values.
Results may differ from the reference program's by a relative error of at most 0.018.
Values are sent between devices in bfloat16 or wider.
A program may use at most 1.5 GiB of HBM per device.

```python
import jax
import jax.numpy as jnp
from jax import lax

SEQUENCES = 64
TOKENS = 2048
D = 1024
FF = 6144
LAYERS = 2
NAMES = ("w_gate", "w_up", "w_down")
SHAPES = {"w_gate": (LAYERS, D, FF), "w_up": (LAYERS, D, FF), "w_down": (LAYERS, FF, D)}


def bump(key, n, height):
    away = (jnp.arange(n, dtype=jnp.int32) - jax.random.randint(key, (), 0, n, jnp.int32)) % n
    return jnp.where(away < n // 8, height, 1.0)


def together(key, own, strength):
    shared = jax.random.normal(key, own.shape[1:], jnp.float32)
    return (own + strength * shared) * lax.rsqrt(1 + strength * strength)


def setup_inputs(seed: int = 0, part: int = 0) -> dict:
    kx, kdy, ka, kb, kz, kf, kh, kl, *kw = jax.random.split(jax.random.key(seed), 8 + len(NAMES))
    kx, kdy, ka, kb = (jax.random.fold_in(k, part) for k in (kx, kdy, ka, kb))
    shape = (SEQUENCES, TOKENS, D)
    much_x, much_dy = jax.random.uniform(kz, (2,), jnp.float32, 0.0, 1.0)
    layers = 2.0 ** jax.random.uniform(kl, (LAYERS, 1, 1), jnp.float32, -1.0, 1.0)
    x = together(ka, jax.random.normal(kx, shape, jnp.float32), much_x) * bump(kf, D, 4.0)
    dy = together(kb, jax.random.normal(kdy, shape, jnp.float32), much_dy)
    drawn = {"x": x.astype(jnp.bfloat16), "dy": (dy * (SEQUENCES * TOKENS) ** -0.5).astype(jnp.bfloat16)}
    for key, name in zip(kw, NAMES, strict=True):
        w = jax.random.normal(key, SHAPES[name], jnp.float32) * SHAPES[name][1] ** -0.5
        drawn[name] = (w * {"w_gate": 1.0, "w_up": bump(kh, FF, 4.0), "w_down": layers}[name]).astype(jnp.bfloat16)
    return drawn


def matmul(a, w):
    return jnp.dot(a, w, preferred_element_type=jnp.float32).astype(jnp.bfloat16)


def normed(h):
    wide = h.astype(jnp.float32)
    scale = lax.rsqrt(jnp.mean(wide**2, -1, keepdims=True) + 1e-6)
    return (wide * scale).astype(jnp.bfloat16)


def layer(h, w):
    a = normed(h)
    gate = jnp.dot(a, w["w_gate"], preferred_element_type=jnp.float32)
    up = jnp.dot(a, w["w_up"], preferred_element_type=jnp.float32)
    return h + matmul((jax.nn.silu(gate) * up).astype(jnp.bfloat16), w["w_down"])


def stack(weights, h):
    return lax.scan(lambda h, w: (layer(h, w), None), h, weights)[0]


def reference(x, dy, w_gate, w_up, w_down):
    weights = dict(zip(NAMES, (w_gate, w_up, w_down), strict=True))

    def take(so_far, sequence):
        h, by_y = sequence
        _, back = jax.vjp(stack, weights, h)
        by_weights, by_h = back(by_y)
        return jax.tree.map(lambda total, term: total + term.astype(jnp.float32), so_far, by_weights), by_h

    none_yet = {name: jnp.zeros(w.shape, jnp.float32) for name, w in weights.items()}
    by_weights, by_x = lax.scan(take, none_yet, (x, dy))
    return (by_x, *(by_weights[name].astype(jnp.bfloat16) for name in NAMES))
```

```python
import jax
import jax.numpy as jnp
from jax import lax
from jax.sharding import PartitionSpec as P

BF, F32 = jnp.bfloat16, jnp.float32
LAYERS = 2


def dot(a, b, dims):
    return lax.dot_general(a, b, (dims, ((), ())), preferred_element_type=F32)


def gather(w):
    half = w.shape[0] // 2
    mine = lax.dynamic_slice_in_dim(w, lax.axis_index("rep") * half, half, 0)
    return lax.all_gather(mine, ("dp", "rep"), axis=0, tiled=True)


def scatter(term):
    return lax.psum_scatter(term.astype(BF), "dp", scatter_dimension=0, tiled=True)


def scale_of(h):
    wide = h.astype(F32)
    return lax.rsqrt(jnp.mean(wide * wide, -1, keepdims=True) + 1e-6)


def body(x, dy, w_gate, w_up, w_down):
    h, g = x[0], dy[0]
    weights = [[gather(w[n]) for w in (w_gate, w_up, w_down)] for n in range(LAYERS)]
    saved = []
    for n in range(LAYERS):
        wg, wu, wd = weights[n]
        s = scale_of(h)
        a = (h.astype(F32) * s).astype(BF)
        gate = dot(a, wg, ((1,), (0,)))
        up = dot(a, wu, ((1,), (0,)))
        hid = (jax.nn.silu(gate) * up).astype(BF)
        saved.append((h, s, a, gate, up, hid))
        if n < LAYERS - 1:
            h = h + dot(hid, wd, ((1,), (0,))).astype(BF)
    grads = [None] * LAYERS
    for n in reversed(range(LAYERS)):
        wg, wu, wd = weights[n]
        h, s, a, gate, up, hid = saved[n]
        d_wd = scatter(dot(hid, g, ((0,), (0,))))
        d_hid = dot(g, wd, ((1,), (1,))).astype(BF).astype(F32)
        sig = jax.nn.sigmoid(gate)
        d_gate = (d_hid * up * (sig * (1 + gate * (1 - sig)))).astype(BF)
        d_up = (d_hid * (gate * sig)).astype(BF)
        d_wg = scatter(dot(a, d_gate, ((0,), (0,))))
        d_wu = scatter(dot(a, d_up, ((0,), (0,))))
        d_a = (dot(d_gate, wg, ((1,), (1,))) + dot(d_up, wu, ((1,), (1,)))).astype(BF).astype(F32)
        wide = h.astype(F32)
        inner = jnp.sum(d_a * wide, -1, keepdims=True) * (s * s * s / h.shape[-1])
        g = g + (d_a * s - wide * inner).astype(BF)
        grads[n] = (d_wg, d_wu, d_wd)
    return (g[None], *(jnp.stack(t) for t in zip(*grads)))


def solution(mesh):
    seq, row = P(("rep", "dp")), P(None, "dp")
    out = P("rep", "dp")
    return jax.shard_map(body, mesh=mesh, in_specs=(seq, seq, row, row, row), out_specs=(seq, out, out, out), check_vma=False)
```

```python
import functools

import jax
import jax.numpy as jnp
from jax import lax
from jax.experimental import pallas as pl
from jax.experimental.pallas import tpu as pltpu
from jax.sharding import PartitionSpec as P

BF, F32 = jnp.bfloat16, jnp.float32
MESH = pl.DeviceIdType.MESH
LAYERS = 2
N = 4
STRIDE = (N * N, N, 1)
NN, NT = ((1,), (0,)), ((1,), (1,))
ALL = slice(None)
VMEM_LIMIT = 66 * 1024 * 1024


def dot(a, b, dims=NN):
    return lax.dot_general(a, b, (dims, ((), ())), preferred_element_type=F32)


def place():
    d = lax.axis_index("dp")
    return d // (N * N), lax.rem(d // N, N), lax.rem(d, N)


def along(v, step):
    return lax.rem(v + step + N, N)


def neighbour(axis, step):
    d, v = lax.axis_index("dp"), place()[axis]
    return {"dp": d + (along(v, step) - v) * STRIDE[axis]}


def meet(partner):
    barrier = pltpu.get_barrier_semaphore()
    peers = [neighbour(axis, step) for axis in range(3) for step in (1, -1)]
    if partner:
        peers.append({"rep": 1 - lax.axis_index("rep")})
    for peer in peers:
        pl.semaphore_signal(barrier, inc=1, device_id=peer, device_id_type=MESH)
    pl.semaphore_wait(barrier, len(peers))


class Gather:
    STAGES = 8

    def __init__(self, mine, whole, sems):
        self.mine, self.whole = mine, whole
        self.send, self.recv, self.local = sems

    @staticmethod
    def scratch():
        return [pltpu.SemaphoreType.DMA((9 * 4 + 3 * 4,)), pltpu.SemaphoreType.DMA((9 * 4 + 3 * 4,)), pltpu.SemaphoreType.DMA((3,))]

    def cols(self, c):
        width = self.mine.shape[-1] // 6
        return pl.ds(pl.multiple_of((lax.axis_index("rep") * 3 + c) * width, width), width)

    def chunk(self, p, c, v, h):
        idx = list(place())
        for k in range(p):
            idx[(c + k) % 3] = ALL
        idx[(c + p) % 3] = v
        return self.whole.at[(h, *idx, ALL, self.cols(c))]

    def copy(self, p, c, slot):
        axis = (c + p) % 3
        v = place()[axis]
        own, left, right, far = v, along(v, -1), along(v, 1), along(v, 2)
        both = slice(0, 2)
        sent, h, to = {0: (own, both, 1), 1: (own, both, -1), 2: (left, 0, 1), 3: (right, 1, -1),
                       4: (own, both, 0), 5: (left, both, 0), 6: (right, both, 0), 7: (far, both, 0)}[slot]
        n = (p * 3 + c) * 4 + slot if slot < 4 else 36 + c * 4 + slot - 4
        dst = self.chunk(p, c, sent, h)
        src = self.mine.at[:, :, self.cols(c)] if p == 0 and slot < 2 else dst
        device = neighbour(axis, to) if to else {"rep": 1 - lax.axis_index("rep")}
        return pltpu.make_async_remote_copy(src_ref=src, dst_ref=dst, send_sem=self.send.at[n], recv_sem=self.recv.at[n],
                                            device_id=device, device_id_type=MESH)

    def keep(self, c):
        return pltpu.make_async_copy(self.mine.at[:, :, self.cols(c)], self.whole.at[(ALL, *place(), ALL, self.cols(c))], self.local.at[c])

    def start(self, p, *slots):
        for slot in slots:
            for c in range(3):
                self.copy(p, c, slot).start()

    def wait(self, p, *slots):
        for slot in slots:
            for c in range(3):
                self.copy(p, c, slot).wait_recv()

    def before(self, s):
        p, part = divmod(s - 1, 2)
        if s == 7:
            self.wait(2, 4, 5, 6, 7)
            for p in range(3):
                for slot in range(8 if p == 2 else 4):
                    for c in range(3):
                        self.copy(p, c, slot).wait_send()
        elif s > 0:
            self.wait(p, *((0, 1) if part == 0 else (2, 3)))
            if s == 2:
                for c in range(3):
                    self.keep(c).wait()

    def after(self, s):
        if s == 0:
            self.start(0, 0, 1)
            for c in range(3):
                self.keep(c).start()
        elif s < 7:
            p, part = divmod(s - 1, 2)
            if part == 0:
                self.start(p, 2, 3)
                if p == 2:
                    self.start(2, 5, 6)
            elif p < 2:
                self.start(p + 1, 0, 1)
                if p == 1:
                    self.start(2, 4)
            else:
                self.start(2, 7)


class Scatter:
    STAGES = 7

    def __init__(self, term, out, refs, by_rows):
        self.term, self.out, self.by_rows = term, out, by_rows
        *bufs, self.own, self.part, self.send, self.recv, self.local = refs
        self.bufs = bufs

    @staticmethod
    def scratch(width):
        piece = (16, width)
        return [
            pltpu.VMEM((3, 6, N, N, *piece), BF), pltpu.VMEM((3, 6, N, *piece), BF), pltpu.VMEM((3, 6, *piece), BF),
            pltpu.VMEM((3, 4, N, N, *piece), BF), pltpu.VMEM((3, 2, N, *piece), BF),
            pltpu.SemaphoreType.DMA((54,)), pltpu.SemaphoreType.DMA((54,)), pltpu.SemaphoreType.DMA((12,)),
        ]

    def piece(self, c, h):
        rows, width = self.bufs[0].shape[-2:]
        n = 2 * c + h
        return (slice(n * rows, (n + 1) * rows), ALL) if self.by_rows else (ALL, slice(n * width, (n + 1) * width))

    def value(self, p, c, v, h):
        if p == 0:
            idx = [ALL] * 3
            idx[c] = v
            return self.term.at[(*idx, *self.piece(c, h))]
        if p == 1:
            rest = [k for k in range(3) if k != c]
            idx = [ALL] * 2
            idx[rest.index((c + 1) % 3)] = v
            return self.own.at[(c, 2 + h, *idx)]
        return self.part.at[c, h, v]

    def copy(self, p, c, slot):
        axis = (c + p) % 3
        v = place()[axis]
        at, h, to = {0: (2, 0, 1), 1: (2, 1, -1), 2: (1, 0, 1), 3: (1, 1, 1), 4: (-1, 0, -1), 5: (-1, 1, -1)}[slot]
        buf = self.bufs[p]
        src = buf.at[c, {2: 0, 5: 1}[slot]] if slot in (2, 5) else self.value(p, c, along(v, at), h)
        n = (p * 3 + c) * 6 + slot
        return pltpu.make_async_remote_copy(src_ref=src, dst_ref=buf.at[c, slot], send_sem=self.send.at[n], recv_sem=self.recv.at[n],
                                            device_id=neighbour(axis, to), device_id_type=MESH)

    def load(self, c, k):
        v = place()[c]
        at, h = ((1, 0), (-1, 1), (0, 0), (0, 1))[k]
        return pltpu.make_async_copy(self.value(0, c, along(v, at), h), self.own.at[c, k], self.local.at[c * 4 + k])

    def held(self, p, c, k):
        if p == 0:
            return self.own.at[c, k]
        v = place()[(c + p) % 3]
        at, h = ((1, 0), (-1, 1), (0, 0), (0, 1))[k]
        return self.value(p, c, along(v, at), h)

    @staticmethod
    def add(dst, *srcs):
        def one(i, _):
            at = (i,) if len(dst.shape) > 2 else ()
            total = srcs[0][at].astype(F32) if at else srcs[0][...].astype(F32)
            for src in srcs[1:]:
                total += (src[at] if at else src[...]).astype(F32)
            if at:
                dst[at] = total.astype(BF)
            else:
                dst[...] = total.astype(BF)
            return 0

        if len(dst.shape) > 2:
            lax.fori_loop(0, dst.shape[0], one, 0)
        else:
            one(0, 0)

    def before(self, s):
        if s == 0:
            return
        p, part = divmod(s - 1, 2)
        for c in range(3):
            buf = self.bufs[p]
            if part == 0:
                for k in (0, 1):
                    self.copy(p, c, k).wait_recv()
                    if p == 0:
                        self.load(c, k).wait()
                    self.add(buf.at[c, k], buf.at[c, k], self.held(p, c, k))
            else:
                for slot in (2, 3, 4, 5):
                    self.copy(p, c, slot).wait_recv()
                for h in (0, 1):
                    if p == 0:
                        self.load(c, 2 + h).wait()
                    dst = (self.own.at[c, 2 + h], self.part.at[c, h], self.out.at[self.piece(c, h)])[p]
                    self.add(dst, self.held(p, c, 2 + h), buf.at[c, 2 + h], buf.at[c, 4 + h])
        if s == 6:
            for p in range(3):
                for c in range(3):
                    for slot in range(6):
                        self.copy(p, c, slot).wait_send()

    def after(self, s):
        p, part = divmod(s, 2)
        if p == 3:
            return
        for slot in (0, 1, 3, 4) if part == 0 else (2, 5):
            for c in range(3):
                self.copy(p, c, slot).start()
        if s == 0:
            for k in range(4):
                for c in range(3):
                    self.load(c, k).start()


def run(engine, steps, step, compute):
    last = max(steps) if steps else -1
    groups = {}
    for s, at in enumerate(steps):
        groups.setdefault(at, []).append(s)
    tail = groups[last][1:] if steps and len(groups[last]) > 1 else []
    for at, stages in groups.items():
        @pl.when(step == at)
        def _(first=stages[0]):
            engine.before(first)
    compute()
    for at, stages in groups.items():
        @pl.when(step == at)
        def _(first=stages[0]):
            engine.after(first)
    if tail:
        @pl.when(step == last)
        def _():
            for s in tail:
                engine.before(s)
                engine.after(s)


def params(**more):
    return pltpu.CompilerParams(vmem_limit_bytes=VMEM_LIMIT, **more)


def whole(shape):
    return pl.BlockSpec(shape, lambda *_: (0,) * len(shape), pipeline_mode=pl.Buffered(1))


ANY = pl.BlockSpec(memory_space=pl.ANY)


def gathered(mine, number):
    two, rows, cols = mine.shape

    def kernel(mine, out, *sems):
        meet(True)
        engine = Gather(mine, out, sems)
        for s in range(Gather.STAGES):
            engine.before(s)
            engine.after(s)

    out = pl.pallas_call(
        kernel, out_shape=jax.ShapeDtypeStruct((two, N, N, N, rows, cols), BF), in_specs=[pl.BlockSpec(memory_space=pltpu.VMEM)], out_specs=ANY,
        scratch_shapes=Gather.scratch(), compiler_params=params(collective_id=number, has_side_effects=True), name="gather",
    )(mine)
    return out.reshape(two, -1, cols)


def forward(a, w, mine, number, tile):
    (tokens, d), ff = a.shape, w.shape[-1]
    n = ff // tile
    steps = [round(t * (n - 1) / 23) for t in (0, 2, 4, 7, 10, 19, 23)] + [n - 1]
    rows = min(tokens, 512)

    def kernel(*refs):
        if mine is None:
            a, w, p, q, hid = refs
        else:
            a, w, own, p, q, hid, nxt, *sems = refs
        step = pl.program_id(0)

        def compute():
            def one(i, _):
                r = pl.ds(pl.multiple_of(i * rows, rows), rows)
                gate = dot(a[r, :], w[0])
                up = dot(a[r, :], w[1])
                sig = jax.nn.sigmoid(gate)
                act = gate * sig
                p[r, :] = act
                q[r, :] = up * (sig * (1 + gate * (1 - sig)))
                hid[r, :] = (act * up).astype(BF)
                return 0

            lax.fori_loop(0, tokens // rows, one, 0)

        if mine is None:
            compute()
        else:
            @pl.when(step == 0)
            def _():
                meet(True)

            run(Gather(own, nxt, sems), steps, step, compute)

    block = pl.BlockSpec((tokens, tile), lambda i: (0, i))
    in_specs = [whole((tokens, d)), pl.BlockSpec((2, d, tile), lambda i: (0, 0, i))]
    out_shape = [jax.ShapeDtypeStruct((tokens, ff), t) for t in (F32, F32, BF)]
    out_specs = [block] * 3
    args, more, scratch = [a, w], {}, []
    if mine is not None:
        in_specs.append(whole(mine.shape))
        out_shape.append(jax.ShapeDtypeStruct((2, N, N, N, *mine.shape[1:]), BF))
        out_specs.append(ANY)
        args.append(mine)
        more, scratch = dict(collective_id=number, has_side_effects=True), Gather.scratch()
    outs = pl.pallas_call(
        kernel, grid=(n,), out_shape=out_shape, in_specs=in_specs, out_specs=out_specs, scratch_shapes=scratch, name="forward",
        compiler_params=params(**more),
        cost_estimate=pl.CostEstimate(flops=4 * tokens * d * ff, bytes_accessed=10 * tokens * ff + 4 * d * ff, transcendentals=tokens * ff),
    )(*args)
    return (*outs[:3], outs[3].reshape(2, -1, ff) if mine is not None else None)


def block_of(term):
    return term.reshape(N, N, N, -1, term.shape[-1])


def width_of(term):
    rows, cols = term.shape[-2:]
    return rows * cols // 96


def hidden_backward(g, gt, at, p, q, hid, wd, term, number, tile):
    (tokens, d), ff = g.shape, p.shape[-1]
    n = ff // tile
    steps = [round(t * (n - 1) / 23) for t in (0, 4, 9, 11, 13, 15, 17)]
    rows, cols = min(tokens, 512), min(d, 512)

    def kernel(*refs):
        if term is None:
            g, gt, at, p, q, hid, wd, dgate, dup, dwg, dwu, dwd = refs
        else:
            g, gt, at, p, q, hid, wd, summand, dgate, dup, dwg, dwu, dwd, summed, *scratch = refs
        step = pl.program_id(0)

        def compute():
            def one(i, _):
                r = pl.ds(pl.multiple_of(i * rows, rows), rows)
                dh = dot(g[r, :], wd[...], NT).astype(BF).astype(F32)
                dup[r, :] = (dh * p[r, :]).astype(BF)
                dgate[r, :] = (dh * q[r, :]).astype(BF)
                return 0

            lax.fori_loop(0, tokens // rows, one, 0)

            def two(i, _):
                m = pl.ds(pl.multiple_of(i * cols, cols), cols)
                dwd[:, m] = dot(gt[m, :], hid[...]).astype(BF).T
                dwg[m, :] = dot(at[m, :], dgate[...]).astype(BF)
                dwu[m, :] = dot(at[m, :], dup[...]).astype(BF)
                return 0

            lax.fori_loop(0, d // cols, two, 0)

        if term is None:
            compute()
        else:
            @pl.when(step == 0)
            def _():
                meet(False)

            run(Scatter(summand, summed, scratch, False), steps, step, compute)

    by_col = pl.BlockSpec((tokens, tile), lambda i: (0, i))
    narrow = pl.BlockSpec((d, tile), lambda i: (0, i))
    by_row = pl.BlockSpec((tile, d), lambda i: (i, 0))
    in_specs = [whole((tokens, d)), whole((d, tokens)), whole((d, tokens)), by_col, by_col, by_col, by_row]
    out_shape = [jax.ShapeDtypeStruct(s, BF) for s in ((tokens, ff), (tokens, ff), (d, ff), (d, ff), (ff, d))]
    out_specs = [by_col, by_col, narrow, narrow, by_row]
    args, more, scratch = [g, gt, at, p, q, hid, wd], {}, []
    if term is not None:
        in_specs.append(ANY)
        args.append(block_of(term))
        out_shape.append(jax.ShapeDtypeStruct(args[-1].shape[-2:], BF))
        out_specs.append(whole(args[-1].shape[-2:]))
        more, scratch = dict(collective_id=number, has_side_effects=True), Scatter.scratch(width_of(args[-1]))
    outs = pl.pallas_call(
        kernel, grid=(n,), out_shape=out_shape, in_specs=in_specs, out_specs=out_specs, scratch_shapes=scratch, name="hidden_backward",
        compiler_params=params(**more),
        cost_estimate=pl.CostEstimate(flops=8 * tokens * d * ff, bytes_accessed=14 * tokens * ff + 8 * d * ff, transcendentals=0),
    )(*args)
    return outs if term is not None else (*outs, None)


def input_backward(dgate, dup, w, term, by_rows, number, tile):
    (tokens, ff), d = dgate.shape, w.shape[1]
    n = ff // tile
    steps = [round(t * (n - 1) / 23) for t in (0, 6, 15, 18, 21, 23)] + [n - 1]
    rows = min(tokens, 512)
    term = block_of(term)

    def kernel(dgate, dup, w, summand, out, summed, acc, *scratch):
        step = pl.program_id(0)

        @pl.when(step == 0)
        def _():
            meet(False)

        def compute():
            def one(i, _):
                r = pl.ds(pl.multiple_of(i * rows, rows), rows)
                new = dot(dgate[r, :], w[0], NT) + dot(dup[r, :], w[1], NT)

                @pl.when(step == 0)
                def _():
                    acc[r, :] = new

                @pl.when(step > 0)
                def _():
                    acc[r, :] += new

                return 0

            lax.fori_loop(0, tokens // rows, one, 0)

            @pl.when(step == n - 1)
            def _():
                out[...] = acc[...].astype(BF)

        run(Scatter(summand, summed, scratch, by_rows), steps, step, compute)

    by_col = pl.BlockSpec((tokens, tile), lambda i: (0, i))
    return pl.pallas_call(
        kernel, grid=(n,), out_shape=[jax.ShapeDtypeStruct((tokens, d), BF), jax.ShapeDtypeStruct(term.shape[-2:], BF)],
        in_specs=[by_col, by_col, pl.BlockSpec((2, d, tile), lambda i: (0, 0, i)), ANY],
        out_specs=[whole((tokens, d)), whole(term.shape[-2:])],
        scratch_shapes=[pltpu.VMEM((tokens, d), F32), *Scatter.scratch(width_of(term))], name="input_backward",
        compiler_params=params(collective_id=number, has_side_effects=True),
        cost_estimate=pl.CostEstimate(flops=4 * tokens * d * ff, bytes_accessed=4 * tokens * ff + 4 * d * ff, transcendentals=0),
    )(dgate, dup, w, term)


def scattered(terms, by_rows, number):
    terms = [block_of(t) for t in terms]
    k = len(terms)
    shapes = [Scatter.scratch(width_of(t)) for t in terms]
    size = len(shapes[0])

    def kernel(*refs):
        meet(False)
        engines = [Scatter(refs[j], refs[k + j], refs[2 * k + j * size:2 * k + (j + 1) * size], by_rows[j]) for j in range(k)]
        for s in range(Scatter.STAGES):
            for engine in engines:
                engine.before(s)
                engine.after(s)

    return pl.pallas_call(
        kernel, out_shape=[jax.ShapeDtypeStruct(t.shape[-2:], BF) for t in terms], in_specs=[ANY] * k,
        out_specs=[pl.BlockSpec(memory_space=pltpu.VMEM)] * k, scratch_shapes=sum(shapes, []), name="scatter",
        compiler_params=params(collective_id=number, has_side_effects=True),
    )(*terms)


def scale_of(h):
    wide = h.astype(F32)
    return lax.rsqrt(jnp.mean(wide * wide, -1, keepdims=True) + 1e-6)


def normed(h, s):
    return (h.astype(F32) * s).astype(BF)


def norm_backward(g, h, s, d_a):
    wide, d_a = h.astype(F32), d_a.astype(F32)
    inner = jnp.sum(d_a * wide, -1, keepdims=True) * (s * s * s / h.shape[-1])
    return g + (d_a * s - wide * inner).astype(BF)


def fetch(w):
    half = w.shape[0] // 2
    mine = lax.dynamic_slice_in_dim(w, lax.axis_index("rep") * half, half, 0)
    return lax.all_gather(mine, ("dp", "rep"), axis=0, tiled=True)


def body(tile, x, dy, w_gate, w_up, w_down):
    x, dy = x[0], dy[0]
    mine = [jnp.stack([w_gate[n], w_up[n]]) for n in range(LAYERS)]
    w0 = gathered(mine[0], 1)
    wd0, wd1 = fetch(w_down[0]), fetch(w_down[1])

    s0 = scale_of(x)
    a0 = normed(x, s0)
    p0, q0, hid0, w1 = forward(a0, w0, mine[1], 2, tile)
    h1 = x + dot(hid0, wd0).astype(BF)
    s1 = scale_of(h1)
    a1 = normed(h1, s1)
    p1, q1, hid1, _ = forward(a1, w1, None, None, tile)

    dgate, dup, t_wg1, t_wu1, t_wd1, _ = hidden_backward(dy, dy.T, a1.T, p1, q1, hid1, wd1, None, None, tile)
    g_wd1 = lax.psum_scatter(t_wd1, "dp", scatter_dimension=0, tiled=True)
    d_a, g_wg1 = input_backward(dgate, dup, w1, t_wg1, False, 3, tile)
    g = norm_backward(dy, h1, s1, d_a)

    dgate, dup, t_wg0, t_wu0, t_wd0, g_wu1 = hidden_backward(g, g.T, a0.T, p0, q0, hid0, wd0, t_wu1, 4, tile)
    d_a, g_wd0 = input_backward(dgate, dup, w0, t_wd0, True, 5, tile)
    g_wg0, g_wu0 = scattered([t_wg0, t_wu0], [False, False], 6)
    by_x = norm_backward(g, x, s0, d_a)
    return by_x[None], jnp.stack([g_wg0, g_wg1]), jnp.stack([g_wu0, g_wu1]), jnp.stack([g_wd0, g_wd1])


def solution(mesh):
    seq, row, out = P(("rep", "dp")), P(None, "dp"), P("rep", "dp")
    return jax.shard_map(functools.partial(body, 256), mesh=mesh, in_specs=(seq, seq, row, row, row), out_specs=(seq, out, out, out),
                         check_vma=False)
```

```python
import functools

import jax
import jax.numpy as jnp
from jax import lax
from jax.experimental import pallas as pl
from jax.experimental.pallas import tpu as pltpu
from jax.sharding import PartitionSpec as P

BF, F32 = jnp.bfloat16, jnp.float32
MESH = pl.DeviceIdType.MESH
LAYERS = 2
N = 4
STRIDE = (N * N, N, 1)
NN, NT = ((1,), (0,)), ((1,), (1,))
ALL = slice(None)
VMEM_LIMIT = 67043328
CHUNK = 512


def dot(a, b, dims=NN):
    return lax.dot_general(a, b, (dims, ((), ())), preferred_element_type=F32)


def place():
    d = lax.axis_index("dp")
    return d // (N * N), lax.rem(d // N, N), lax.rem(d, N)


def along(v, step):
    return lax.rem(v + step + N, N)


def neighbour(axis, step):
    d, v = lax.axis_index("dp"), place()[axis]
    return {"dp": d + (along(v, step) - v) * STRIDE[axis]}


def meet(partner):
    barrier = pltpu.get_barrier_semaphore()
    peers = [neighbour(axis, step) for axis in range(3) for step in (1, -1)]
    if partner:
        peers.append({"rep": 1 - lax.axis_index("rep")})
    for peer in peers:
        pl.semaphore_signal(barrier, inc=1, device_id=peer, device_id_type=MESH)
    pl.semaphore_wait(barrier, len(peers))


class Gather:
    STAGES = 8

    def __init__(self, mine, whole, sems, by_rows=False):
        self.mine, self.whole, self.by_rows = mine, whole, by_rows
        self.send, self.recv, self.local = sems

    @staticmethod
    def scratch():
        return [pltpu.SemaphoreType.DMA((9 * 4 + 3 * 4,)), pltpu.SemaphoreType.DMA((9 * 4 + 3 * 4,)), pltpu.SemaphoreType.DMA((3,))]

    def piece(self, c, h=None):
        n = lax.axis_index("rep") * 3 + c
        rows, cols = self.mine.shape
        if self.by_rows:
            part = ALL if h is None else slice(h * cols // 2, (h + 1) * cols // 2)
            return pl.ds(pl.multiple_of(n * (rows // 6), rows // 6), rows // 6), part
        width = cols // 12
        return ALL, pl.ds(pl.multiple_of((2 * n + (h or 0)) * width, width), 2 * width if h is None else width)

    def chunk(self, p, c, v, h):
        idx = list(place())
        for k in range(p):
            idx[(c + k) % 3] = ALL
        idx[(c + p) % 3] = v
        return self.whole.at[(*idx, *self.piece(c, h))]

    def copy(self, p, c, slot):
        axis = (c + p) % 3
        v = place()[axis]
        own, left, right, far = v, along(v, -1), along(v, 1), along(v, 2)
        sent, h, to = {0: (own, None, 1), 1: (own, None, -1), 2: (left, 0, 1), 3: (right, 1, -1),
                       4: (own, None, 0), 5: (left, None, 0), 6: (right, None, 0), 7: (far, None, 0)}[slot]
        n = (p * 3 + c) * 4 + slot if slot < 4 else 36 + c * 4 + slot - 4
        dst = self.chunk(p, c, sent, h)
        src = self.mine.at[self.piece(c)] if p == 0 and slot < 2 else dst
        device = neighbour(axis, to) if to else {"rep": 1 - lax.axis_index("rep")}
        return pltpu.make_async_remote_copy(src_ref=src, dst_ref=dst, send_sem=self.send.at[n], recv_sem=self.recv.at[n],
                                            device_id=device, device_id_type=MESH)

    def keep(self, c):
        return pltpu.make_async_copy(self.mine.at[self.piece(c)], self.whole.at[(*place(), *self.piece(c))], self.local.at[c])

    def start(self, p, *slots):
        for slot in slots:
            for c in range(3):
                self.copy(p, c, slot).start()

    def wait(self, p, *slots):
        for slot in slots:
            for c in range(3):
                self.copy(p, c, slot).wait_recv()

    def before(self, s):
        p, part = divmod(s - 1, 2)
        if s == 7:
            self.wait(2, 4, 5, 6, 7)
            for p in range(3):
                for slot in range(8 if p == 2 else 4):
                    for c in range(3):
                        self.copy(p, c, slot).wait_send()
        elif s > 0:
            self.wait(p, *((0, 1) if part == 0 else (2, 3)))
            if s == 2:
                for c in range(3):
                    self.keep(c).wait()

    def after(self, s):
        if s == 0:
            self.start(0, 0, 1)
            for c in range(3):
                self.keep(c).start()
        elif s < 7:
            p, part = divmod(s - 1, 2)
            if part == 0:
                self.start(p, 2, 3)
                if p == 2:
                    self.start(2, 5, 6)
            elif p < 2:
                self.start(p + 1, 0, 1)
                if p == 1:
                    self.start(2, 4)
            else:
                self.start(2, 7)


class Scatter:
    STAGES = 7

    def __init__(self, term, out, refs):
        self.term, self.out, self.pair = term, out, len(out.shape) == 3
        *bufs, self.own, self.part, self.send, self.recv, self.local = refs
        self.bufs = bufs

    @staticmethod
    def scratch(width):
        piece = (16, width)
        return [
            pltpu.VMEM((3, 6, N, N, *piece), BF), pltpu.VMEM((3, 6, N, *piece), BF), pltpu.VMEM((3, 6, *piece), BF),
            pltpu.VMEM((3, 4, N, N, *piece), BF), pltpu.VMEM((3, 2, N, *piece), BF),
            pltpu.SemaphoreType.DMA((54,)), pltpu.SemaphoreType.DMA((54,)), pltpu.SemaphoreType.DMA((12,)),
        ]

    def piece(self, c, h, idx=()):
        rows, width = self.bufs[0].shape[-2:]
        if self.pair:
            return h, *idx, ALL, slice(c * width, (c + 1) * width)
        n = 2 * c + h
        return *idx, slice(n * rows, (n + 1) * rows), ALL

    def value(self, p, c, v, h):
        if p == 0:
            idx = [ALL] * 3
            idx[c] = v
            return self.term.at[self.piece(c, h, idx)]
        if p == 1:
            rest = [k for k in range(3) if k != c]
            idx = [ALL] * 2
            idx[rest.index((c + 1) % 3)] = v
            return self.own.at[(c, 2 + h, *idx)]
        return self.part.at[c, h, v]

    def copy(self, p, c, slot):
        axis = (c + p) % 3
        v = place()[axis]
        at, h, to = {0: (2, 0, 1), 1: (2, 1, -1), 2: (1, 0, 1), 3: (1, 1, 1), 4: (-1, 0, -1), 5: (-1, 1, -1)}[slot]
        buf = self.bufs[p]
        src = buf.at[c, {2: 0, 5: 1}[slot]] if slot in (2, 5) else self.value(p, c, along(v, at), h)
        n = (p * 3 + c) * 6 + slot
        return pltpu.make_async_remote_copy(src_ref=src, dst_ref=buf.at[c, slot], send_sem=self.send.at[n], recv_sem=self.recv.at[n],
                                            device_id=neighbour(axis, to), device_id_type=MESH)

    def load(self, c, k):
        v = place()[c]
        at, h = ((1, 0), (-1, 1), (0, 0), (0, 1))[k]
        return pltpu.make_async_copy(self.value(0, c, along(v, at), h), self.own.at[c, k], self.local.at[c * 4 + k])

    def held(self, p, c, k):
        if p == 0:
            return self.own.at[c, k]
        v = place()[(c + p) % 3]
        at, h = ((1, 0), (-1, 1), (0, 0), (0, 1))[k]
        return self.value(p, c, along(v, at), h)

    @staticmethod
    def add(dst, *srcs):
        def one(i, _):
            at = (i,) if len(dst.shape) > 2 else ()
            total = srcs[0][at].astype(F32) if at else srcs[0][...].astype(F32)
            for src in srcs[1:]:
                total += (src[at] if at else src[...]).astype(F32)
            if at:
                dst[at] = total.astype(BF)
            else:
                dst[...] = total.astype(BF)
            return 0

        if len(dst.shape) > 2:
            lax.fori_loop(0, dst.shape[0], one, 0)
        else:
            one(0, 0)

    def before(self, s):
        if s == 0:
            return
        p, part = divmod(s - 1, 2)
        for c in range(3):
            buf = self.bufs[p]
            if part == 0:
                for k in (0, 1):
                    self.copy(p, c, k).wait_recv()
                    if p == 0:
                        self.load(c, k).wait()
                    self.add(buf.at[c, k], buf.at[c, k], self.held(p, c, k))
            else:
                for slot in (2, 3, 4, 5):
                    self.copy(p, c, slot).wait_recv()
                for h in (0, 1):
                    if p == 0:
                        self.load(c, 2 + h).wait()
                    dst = (self.own.at[c, 2 + h], self.part.at[c, h], self.out.at[self.piece(c, h)])[p]
                    self.add(dst, self.held(p, c, 2 + h), buf.at[c, 2 + h], buf.at[c, 4 + h])
        if s == 6:
            for p in range(3):
                for c in range(3):
                    for slot in range(6):
                        self.copy(p, c, slot).wait_send()

    def after(self, s):
        p, part = divmod(s, 2)
        if p == 3:
            return
        for slot in (0, 1, 3, 4) if part == 0 else (2, 5):
            for c in range(3):
                self.copy(p, c, slot).start()
        if s == 0:
            for k in range(4):
                for c in range(3):
                    self.load(c, k).start()


def run(engines, steps, step, last, compute):
    def go(s):
        for engine in engines:
            engine.before(s)
            engine.after(s)

    for s, at in enumerate(steps):
        if at <= last:
            pl.when(step == at)(functools.partial(go, s))
    compute()

    @pl.when(step == last)
    def _():
        for s, at in enumerate(steps):
            if at > last:
                go(s)


def params(**more):
    return pltpu.CompilerParams(vmem_limit_bytes=VMEM_LIMIT, **more)


def whole(shape):
    return pl.BlockSpec(shape, lambda *_: (0,) * len(shape), pipeline_mode=pl.Buffered(1))


ANY = pl.BlockSpec(memory_space=pl.ANY)


def rows_of(tokens):
    size = min(tokens, CHUNK)
    return [pl.ds(i, size) for i in range(0, tokens, size)]


def gathered(wanted, x, number):
    k = len(wanted)

    def kernel(*refs):
        mine, (x, *refs) = refs[:k], refs[k:]
        outs, (a, *sems) = refs[:k], refs[k:]
        meet(True)
        engines = gathers(wanted, mine, outs, sems)
        for s in range(Gather.STAGES):
            for engine in engines:
                engine.before(s)
                engine.after(s)
            if s == 4:
                def one(i, _):
                    r = pl.ds(pl.multiple_of(i * 64, 64), 64)
                    h = x[r, :]
                    a[r, :] = normed(h, scale_of(h))
                    return 0

                lax.fori_loop(0, x.shape[0] // 64, one, 0)

    vmem = pl.BlockSpec(memory_space=pltpu.VMEM)
    arrays, _, shapes, specs, scratch = fetching(wanted)
    *outs, a = pl.pallas_call(
        kernel, out_shape=[*shapes, jax.ShapeDtypeStruct(x.shape, BF)], in_specs=[vmem] * (k + 1), out_specs=[*specs, vmem],
        scratch_shapes=scratch, name="gather", compiler_params=params(collective_id=number, has_side_effects=True),
    )(*arrays, x)
    return *(out.reshape(-1, out.shape[-1]) for out in outs), a


def fetching(wanted):
    arrays = [w for _, w in wanted]
    return (arrays, [whole(w.shape) for w in arrays], [jax.ShapeDtypeStruct((N, N, N, *w.shape[1:]), BF) for w in arrays], [ANY] * len(arrays),
            Gather.scratch() * len(arrays))


def gathers(wanted, mine, outs, sems):
    return [Gather(mine[j].at[n], outs[j], sems[3 * j:3 * j + 3], w.shape[1] > 16) for j, (n, w) in enumerate(wanted)]


def forward(a, wg, wu, flips, wanted, number, tile, steps):
    (tokens, d), ff = a.shape, wg.shape[-1]
    n, k, m = ff // tile, len(flips), len(wanted)
    wide = min(tokens, 128)

    def kernel(*refs):
        a, wg, wu, *refs = refs
        flips, refs = refs[:k], refs[k:]
        own, (p, q, hid, *refs) = refs[:m], refs[m:]
        flipped, refs = refs[:k], refs[k:]
        step = pl.program_id(0)

        def compute():
            for src, dst in zip(flips, flipped):
                r = pl.ds(pl.multiple_of(lax.rem(step, tokens // wide) * wide, wide), wide)
                dst[:, r] = src[r, :].T
            for r in rows_of(tokens):
                gate = dot(a[r, :], wg[...])
                up = dot(a[r, :], wu[...])
                sig = jax.nn.sigmoid(gate)
                act = gate * sig
                p[r, :] = act
                q[r, :] = up * (sig * (1 + gate * (1 - sig)))
                hid[r, :] = (act * up).astype(BF)

        if not wanted:
            compute()
        else:
            @pl.when(step == 0)
            def _():
                meet(True)

            run(gathers(wanted, own, refs[:m], refs[m:]), steps, step, n - 1, compute)

    assert n >= tokens // wide
    block = pl.BlockSpec((tokens, tile), lambda i: (0, i))
    narrow = pl.BlockSpec((d, tile), lambda i: (0, i))
    in_specs = [whole((tokens, d)), narrow, narrow] + [whole((tokens, d))] * k
    out_shape = [jax.ShapeDtypeStruct((tokens, ff), t) for t in (F32, F32, BF)] + [jax.ShapeDtypeStruct((d, tokens), BF)] * k
    out_specs = [block] * 3 + [whole((d, tokens))] * k
    arrays, *new, scratch = fetching(wanted)
    outs = pl.pallas_call(
        kernel, grid=(n,), out_shape=out_shape + new[1], in_specs=in_specs + new[0], out_specs=out_specs + new[2], scratch_shapes=scratch,
        name="forward", compiler_params=params(**(dict(collective_id=number, has_side_effects=True) if wanted else {})),
        cost_estimate=pl.CostEstimate(flops=4 * tokens * d * ff, bytes_accessed=10 * tokens * ff + 4 * d * ff, transcendentals=tokens * ff),
    )(a, wg, wu, *flips, *arrays)
    return (*outs[:3], outs[3:3 + k], [o.reshape(-1, o.shape[-1]) for o in outs[3 + k:]])


def down(hid, wd, h, wanted, number, tile, steps):
    (tokens, ff), d = hid.shape, wd.shape[-1]
    n, m = ff // tile, len(wanted)

    def kernel(hid, wd, h, *refs):
        own, (out, a, *refs) = refs[:m], refs[m:]
        nxt, (acc, *sems) = refs[:m], refs[m:]
        step = pl.program_id(0)

        @pl.when(step == 0)
        def _():
            if wanted:
                meet(True)
            acc[...] = jnp.zeros_like(acc)

        def compute():
            for r in rows_of(tokens):
                acc[r, :] += dot(hid[r, :], wd[...])

            @pl.when(step == n - 1)
            def _():
                def one(i, _):
                    r = pl.ds(pl.multiple_of(i * 64, 64), 64)
                    new = (h[r, :].astype(F32) + acc[r, :].astype(BF).astype(F32)).astype(BF)
                    out[r, :] = new
                    a[r, :] = normed(new, scale_of(new))
                    return 0

                lax.fori_loop(0, tokens // 64, one, 0)

        run(gathers(wanted, own, nxt, sems), steps, step, n - 1, compute)

    in_specs = [pl.BlockSpec((tokens, tile), lambda i: (0, i)), pl.BlockSpec((tile, d), lambda i: (i, 0)), whole((tokens, d))]
    out_shape, out_specs = [jax.ShapeDtypeStruct((tokens, d), BF)] * 2, [whole((tokens, d))] * 2
    arrays, *new, scratch = fetching(wanted)
    outs = pl.pallas_call(
        kernel, grid=(n,), out_shape=out_shape + new[1], in_specs=in_specs + new[0], out_specs=out_specs + new[2],
        scratch_shapes=[pltpu.VMEM((tokens, d), F32), *scratch], name="down",
        compiler_params=params(**(dict(collective_id=number, has_side_effects=True) if wanted else {})),
        cost_estimate=pl.CostEstimate(flops=2 * tokens * d * ff, bytes_accessed=2 * tokens * ff + 2 * d * ff, transcendentals=0),
    )(hid, wd, h, *arrays)
    return (*outs[:2], [o.reshape(-1, o.shape[-1]) for o in outs[2:]])


def block_of(term):
    return term.reshape(*term.shape[:-2], N, N, N, -1, term.shape[-1])


def shape_of(term):
    return term.shape[:-5] + term.shape[-2:]


def buffers(terms):
    return sum((Scatter.scratch(t.shape[-1] // (3 if t.ndim == 6 else 1)) for t in terms), [])


def traffic(ins, outs, scratch):
    size = len(scratch) // max(len(ins), 1)
    return [Scatter(ins[j], outs[j], scratch[j * size:(j + 1) * size]) for j in range(len(ins))]


def hidden_backward(g, gt, at, p, q, hid, wd, span, into, terms, number, tile, steps):
    (tokens, d), ff = g.shape, p.shape[-1]
    first, n = span
    k, m = len(terms), len(into)
    cols = min(d, 512)

    def kernel(g, gt, at, p, q, hid, wd, *refs):
        summands, refs = refs[m:m + k], refs[m + k:]
        dgate, dup, dwd, dw, *refs = refs
        summed, scratch = refs[:k], refs[k:]
        step = pl.program_id(0)

        def compute():
            for r in rows_of(tokens):
                dh = dot(g[r, :], wd[...], NT).astype(BF).astype(F32)
                dup[r, :] = (dh * p[r, :]).astype(BF)
                dgate[r, :] = (dh * q[r, :]).astype(BF)
            for i in range(0, d, cols):
                r = pl.ds(i, cols)
                dwd[:, r] = dot(gt[r, :], hid[...]).astype(BF).T
            for i in range(0, d, cols):
                r = pl.ds(i, cols)
                dw[0, r, :] = dot(at[r, :], dgate[...]).astype(BF)
                dw[1, r, :] = dot(at[r, :], dup[...]).astype(BF)

        if not terms:
            compute()
        else:
            @pl.when(step == 0)
            def _():
                meet(False)

            run(traffic(summands, summed, scratch), steps, step, n - 1, compute)

    by_col = pl.BlockSpec((tokens, tile), lambda i: (0, i + first))
    both = pl.BlockSpec((2, d, tile), lambda i: (0, 0, i))
    by_row = pl.BlockSpec((tile, d), lambda i: (i + first, 0))
    terms = [block_of(t) for t in terms]
    shapes = [shape_of(t) for t in terms]
    return pl.pallas_call(
        kernel, grid=(n,), name="hidden_backward",
        out_shape=[jax.ShapeDtypeStruct(s, BF) for s in ((tokens, ff), (tokens, ff), (ff, d), (2, d, n * tile), *shapes)],
        in_specs=[whole((tokens, d)), whole((d, tokens)), whole((d, tokens)), by_col, by_col, by_col, by_row] + [ANY] * (m + k),
        out_specs=[by_col, by_col, by_row, both] + [whole(s) for s in shapes],
        scratch_shapes=buffers(terms), input_output_aliases={7 + j: j for j in range(m)},
        compiler_params=params(**(dict(collective_id=number, has_side_effects=True) if terms else {})),
        cost_estimate=pl.CostEstimate(flops=8 * tokens * d * n * tile, bytes_accessed=(14 * tokens + 8 * d) * n * tile, transcendentals=0),
    )(g, gt, at, p, q, hid, wd, *into, *terms)


def input_backward(dgate, dup, wg, wu, h, g, terms, number, tile, steps):
    (tokens, ff), d = dgate.shape, wg.shape[0]
    n, k = ff // tile, len(terms)
    size = min(tokens, 256)
    terms = [block_of(t) for t in terms]

    def kernel(dgate, dup, wg, wu, h, g, *refs):
        summands, (out, *refs) = refs[:k], refs[k:]
        summed, (acc, held, sems, *scratch) = refs[:k], refs[k:]
        step = pl.program_id(0)

        @pl.when(step == 0)
        def _():
            if terms:
                meet(False)
            acc[...] = jnp.zeros_like(acc)

        def loads(i):
            r, slot = pl.ds(pl.multiple_of(i * size, size), size), lax.rem(i, 2)
            return [pltpu.make_async_copy(src.at[r, :], held.at[slot, j], sems.at[slot, j]) for j, src in enumerate((h, g))]

        def finish(i, _):
            @pl.when(i + 1 < tokens // size)
            def _():
                for load in loads(i + 1):
                    load.start()

            for load in loads(i):
                load.wait()

            def one(j, _):
                q = pl.ds(pl.multiple_of(j * 64, 64), 64)
                r = pl.ds(pl.multiple_of(i * size + j * 64, 64), 64)
                old, by_new = held[lax.rem(i, 2), 0, q, :], held[lax.rem(i, 2), 1, q, :]
                out[r, :] = norm_backward(by_new, old, scale_of(old), acc[r, :].astype(BF))
                return 0

            lax.fori_loop(0, size // 64, one, 0)
            return 0

        def compute():
            for r in rows_of(tokens):
                acc[r, :] += dot(dgate[r, :], wg[...], NT) + dot(dup[r, :], wu[...], NT)

            @pl.when(step == n - 1)
            def _():
                for load in loads(0):
                    load.start()
                lax.fori_loop(0, tokens // size, finish, 0)

        run(traffic(summands, summed, scratch), steps, step, n - 1, compute)

    by_col = pl.BlockSpec((tokens, tile), lambda i: (0, i))
    narrow = pl.BlockSpec((d, tile), lambda i: (0, i))
    shapes = [shape_of(t) for t in terms]
    return pl.pallas_call(
        kernel, grid=(n,), out_shape=[jax.ShapeDtypeStruct(s, BF) for s in ((tokens, d), *shapes)],
        in_specs=[by_col, by_col, narrow, narrow] + [ANY] * (2 + k),
        out_specs=[whole((tokens, d))] + [whole(s) for s in shapes], name="input_backward",
        scratch_shapes=[pltpu.VMEM((tokens, d), F32), pltpu.VMEM((2, 2, size, d), BF), pltpu.SemaphoreType.DMA((2, 2))]
        + buffers(terms),
        compiler_params=params(**(dict(collective_id=number, has_side_effects=True) if terms else {})),
        cost_estimate=pl.CostEstimate(flops=4 * tokens * d * ff, bytes_accessed=4 * tokens * ff + 4 * d * ff, transcendentals=0),
    )(dgate, dup, wg, wu, h, g, *terms)


def scale_of(h):
    wide = h.astype(F32)
    return lax.rsqrt(jnp.mean(wide * wide, -1, keepdims=True) + 1e-6)


def normed(h, s):
    return (h.astype(F32) * s).astype(BF)


def norm_backward(g, h, s, d_a):
    wide, d_a = h.astype(F32), d_a.astype(F32)
    inner = jnp.sum(d_a * wide, -1, keepdims=True) * (s * s * s / h.shape[-1])
    return (g.astype(F32) + (d_a * s - wide * inner).astype(BF).astype(F32)).astype(BF)


def body(x, dy, w_gate, w_up, w_down):
    x, dy = x[0], dy[0]
    tiles = w_gate.shape[-1] // 256
    first, second = (0, tiles // 2), (tiles // 2, tiles - tiles // 2)
    one, two = (0, 3, 7, 8, 10, 11, 12), (0, 15, 24, 24, 24, 24, 24)

    wg0, wu0, a0 = gathered([(0, w_gate), (0, w_up)], x, 1)
    p0, q0, hid0, (at0,), (wd0, wg1) = forward(a0, wg0, wu0, [a0], [(0, w_down), (1, w_gate)], 2, 256, (0, 2, 4, 6, 9, 19, 23, 24))
    h1, a1, (wu1,) = down(hid0, wd0, x, [(1, w_up)], 3, 512, (0, 2, 3, 5, 7, 12, 12, 12))
    p1, q1, hid1, (at1, dyt), (wd1,) = forward(a1, wg1, wu1, [a1, dy], [(1, w_down)], 4, 256, (0, 2, 5, 8, 11, 18, 21, 23))

    *some, t1a = hidden_backward(dy, dyt, at1, p1, q1, hid1, wd1, first, (), [], None, 256, ())
    dgate, dup, t_wd1, t1b, g1a = hidden_backward(dy, dyt, at1, p1, q1, hid1, wd1, second, some, [t1a], 5, 256, one)
    g, g_wd1 = input_backward(dgate, dup, wg1, wu1, h1, dy, [t_wd1], 6, 512, one)

    gt = g.T
    *some, t0a, g1b = hidden_backward(g, gt, at0, p0, q0, hid0, wd0, first, (), [t1b], 7, 256, one)
    dgate, dup, t_wd0, t0b, g0a = hidden_backward(g, gt, at0, p0, q0, hid0, wd0, second, some, [t0a], 8, 256, one)
    by_x, g_wd0, g0b = input_backward(dgate, dup, wg0, wu0, x, g, [t_wd0, t0b], 9, 256, two)

    by_gate, by_up = jnp.stack([jnp.concatenate([g0a, g0b], -1), jnp.concatenate([g1a, g1b], -1)], 1)
    return by_x[None], by_gate, by_up, jnp.stack([g_wd0, g_wd1])


def solution(mesh):
    seq, row, out = P(("rep", "dp")), P(None, "dp"), P("rep", "dp")
    return jax.shard_map(body, mesh=mesh, in_specs=(seq, seq, row, row, row), out_specs=(seq, out, out, out),
                         check_vma=False)
```
